512 devices in a mesh: groups: 2 (over y), seq: 16 (over z), head: 8 (over x), dim: 2 (over core).
Axes of the slice: x: 8, y: 2, z: 16, core: 2. Of those that a mesh axis runs over, the one named last changes fastest.
The devices are a block of a 8x16x16 slice.
Arguments:
- query: bfloat16 [4, 16, 4096, 128], P('groups', 'head', 'seq'), parts along dimension 0, may hold values from -6 to 6
- key: bfloat16 [4, 16, 4096, 128], P('groups', 'head', 'seq'), parts along dimension 0, may hold values from -6 to 6
- value: bfloat16 [4, 16, 128, 4096], P('groups', 'head', 'dim', 'seq'), parts along dimension 0, may hold values from -6 to 6
- out_gate: bfloat16 [4, 16, 128, 4096], P('groups', 'head', 'dim', 'seq'), parts along dimension 0, may hold values from -6 to 6
- beta: float32 [4, 16, 4096], P('groups', 'head', 'seq'), parts along dimension 0, may hold values from 0.1 to 0.9
- log_decay: float32 [4, 16, 4096], P('groups', 'head', 'seq'), parts along dimension 0, may hold values from -1 to 0, as said below
- lengths: int32 [4, 16], P('groups', 'seq'), parts along dimension 0, may hold values from 128 to 256
- norm_gain: float32 [128], P('dim'), may hold values from 0.1 to 1.9
Outputs:
- output: bfloat16 [4, 16, 128, 4096], P('groups', 'head', 'dim', 'seq'), parts along dimension 0
The draws below stay inside these ranges and needn't reach their ends.
There are 2 independent parts, one for each index of `groups`. The reference program is written for one: setup_inputs(seed, part) draws one part's arguments, and reference() takes and returns one part's arrays. A program takes and returns all parts, laid end to end along the dimension named above; an argument that names none is the same for every part. Nothing has to cross between parts.
Inputs may be any that keep to these rules, and one draw needn't show every extreme that they name: `log_decay`: negative.
All inputs are finite; a program needn't handle non-finite values.
Results may differ from the reference program's by a relative error of at most 0.001.
Values sent between devices are 32-bit elements; how exact they have to be, the bound alone decides.
No kernel may reach another device: no remote copies, remote signals or barrier semaphores. Data moves between devices by JAX's collectives and lax.ppermute only.
A program may use at most 64 MiB of HBM per device.

```python
import math
import jax
import jax.numpy as jnp
from jax import lax

HEAD_COUNT = 16
DK = 128
DV = 128
TILE = 64
WINDOW = 4
TOK_DEV = 256
SEQUENCE_COUNT = 2
TOKEN_COUNT = 4096
N_SEQ = 16


def draw_log_decay(key, part):
    key_rows = jax.random.split(key, 7)
    chain_len = float(WINDOW * TOK_DEV)
    share = 0.5
    quick = jax.random.uniform(key_rows[0], (SEQUENCE_COUNT, HEAD_COUNT, 1)) < share
    fast_rate = jnp.exp(jax.random.uniform(key_rows[1], (SEQUENCE_COUNT, HEAD_COUNT, 1), minval=math.log(1.0 / 50.0), maxval=math.log(1.0 / 25.0)))
    slow_rate = jnp.exp(jax.random.uniform(key_rows[2], (SEQUENCE_COUNT, HEAD_COUNT, 1), minval=math.log(0.05 / chain_len), maxval=math.log(0.5 / chain_len)))
    baseline_rate = jnp.where(quick, fast_rate, slow_rate)
    block_multiplier = jax.random.uniform(key_rows[3], (SEQUENCE_COUNT, HEAD_COUNT, TOKEN_COUNT // TOK_DEV), minval=0.6, maxval=1.4)
    block_multiplier = jnp.repeat(block_multiplier, TOK_DEV, axis=-1)
    coarse_estimate = jax.random.uniform(key_rows[4], (SEQUENCE_COUNT, HEAD_COUNT, TOKEN_COUNT), minval=0.5, maxval=1.5)
    spike_struck = jax.random.uniform(key_rows[5], (SEQUENCE_COUNT, HEAD_COUNT, TOKEN_COUNT)) < 3.0 / TOKEN_COUNT
    spike_length = jax.random.uniform(key_rows[6], (SEQUENCE_COUNT, HEAD_COUNT, TOKEN_COUNT), minval=0.22, maxval=0.69)
    spike_event = jnp.where(spike_struck, spike_length, 0.0)
    return (-(baseline_rate * block_multiplier * coarse_estimate) - spike_event).astype(jnp.float32)


def draw_key(key, part):
    subkeys = jax.random.split(key, 3)
    sub_rank = max(DK // 8, 4)
    side_share = 0.0625
    side_scale = math.sqrt(side_share * DK / (DK - sub_rank - side_share * DK))
    basis_rows = jax.random.normal(subkeys[0], (SEQUENCE_COUNT, HEAD_COUNT, sub_rank, DK), dtype=jnp.float32)
    mixing = jax.random.normal(subkeys[1], (SEQUENCE_COUNT, HEAD_COUNT, TOKEN_COUNT, sub_rank), dtype=jnp.float32)
    spread_part = jax.random.normal(subkeys[2], (SEQUENCE_COUNT, HEAD_COUNT, TOKEN_COUNT, DK), dtype=jnp.float32)
    aligned = jnp.einsum('shtr,shrd->shtd', mixing, basis_rows) / math.sqrt(float(sub_rank))
    return jnp.clip(aligned + side_scale * spread_part, -6.0, 6.0).astype(jnp.bfloat16)


def with_ends(array, stream_key, least, largest):
    index_at = [jax.random.randint(jax.random.fold_in(stream_key, axis), (), 0, length) for axis, length in enumerate(array.shape)]
    main_axis = array.shape.index(max(array.shape))
    neighbour = index_at[:main_axis] + [(index_at[main_axis] + 1) % array.shape[main_axis]] + index_at[main_axis + 1:]
    return array.at[tuple(index_at)].set(least).at[tuple(neighbour)].set(largest)


def level_of(rng, shape, cuts, least, high):
    def one(dim, parts):
        heights = jax.random.uniform(jax.random.fold_in(jax.random.fold_in(rng, 6), dim), (parts,), jnp.float32, least / len(cuts), high / len(cuts))
        return jnp.repeat(jnp.exp(heights), shape[dim] // parts).reshape((-1,) + (1,) * (len(shape) - dim - 1))

    gain = one(*cuts[0])
    for cut in cuts[1:]:
        gain = gain * one(*cut)
    return gain


def normal_values(key, extent, deviation, most, cuts=(), kind=jnp.bfloat16):
    values = deviation * jax.random.normal(key, extent, jnp.float32)
    if cuts:
        values = values * level_of(key, extent, cuts, -0.22, 0.18)
    return jnp.clip(values, -most, most).astype(kind)


def setup_inputs(seed: int = 0, part: int = 0) -> dict:
    arg_keys = jax.random.split(jax.random.key(seed), 9)
    part_keys = jax.random.split(jax.random.fold_in(arg_keys[8], part), 9)
    query = normal_values(part_keys[0], (SEQUENCE_COUNT, HEAD_COUNT, TOKEN_COUNT, DK), 1.0, 6.0, ((1, 8), (2, 16)))
    key = draw_key(jax.random.fold_in(jax.random.fold_in(arg_keys[8], part), 71), part)
    value = normal_values(part_keys[2], (SEQUENCE_COUNT, HEAD_COUNT, DV, TOKEN_COUNT), 1.0, 6.0, ((1, 8), (2, 2), (3, 16)))
    out_gate = normal_values(part_keys[3], (SEQUENCE_COUNT, HEAD_COUNT, DV, TOKEN_COUNT), 1.0, 6.0, ((1, 8), (2, 2), (3, 16)))
    beta = jnp.clip(0.1 + 0.79999997 * jax.random.uniform(part_keys[4], (SEQUENCE_COUNT, HEAD_COUNT, TOKEN_COUNT), jnp.float32) ** level_of(part_keys[4], (SEQUENCE_COUNT, HEAD_COUNT, TOKEN_COUNT), ((1, 8), (2, 16)), -0.2, 0.2), 0.1, 0.9)
    log_decay = draw_log_decay(jax.random.fold_in(jax.random.fold_in(arg_keys[8], part), 71), part)
    lengths = with_ends(jax.random.randint(part_keys[6], (SEQUENCE_COUNT, N_SEQ), TOK_DEV // 2, TOK_DEV + 1), jax.random.fold_in(part_keys[6], 1), TOK_DEV // 2, TOK_DEV).astype(jnp.int32)
    norm_gain = jnp.clip(1.0 + 0.18 * jax.random.normal(arg_keys[7], (DV,), jnp.float32), 0.1, 1.9)
    return {"query": query, "key": key, "value": value, "out_gate": out_gate, "beta": beta, "log_decay": log_decay, "lengths": lengths, "norm_gain": norm_gain}


FULL_PREC = lax.Precision.HIGHEST

def apply_map(left, right):
    return jnp.matmul(left, right, precision=FULL_PREC)

def tile_terms(query_t, unit_t, value_t, eff_rate, eff_decay):
    tile_len = query_t.shape[-2]
    cumlog = jnp.cumsum(eff_decay, axis=-1)
    index_row = jnp.arange(tile_len)
    causal = index_row[:, None] >= index_row[None, :]
    before = index_row[:, None] > index_row[None, :]
    log_gap = cumlog[..., :, None] - cumlog[..., None, :]
    decays = jnp.where(causal, jnp.exp(jnp.where(causal, log_gap, 0.0)), 0.0)
    key_gram = jnp.einsum('...rd,...sd->...rs', unit_t, unit_t, precision=FULL_PREC)
    coupling = jnp.where(before, eff_rate[..., :, None] * decays * key_gram, 0.0)
    identity = jnp.eye(tile_len, dtype=coupling.dtype)
    right_side = jnp.concatenate([jnp.swapaxes(value_t, -1, -2) * eff_rate[..., None], unit_t * (eff_rate * jnp.exp(cumlog))[..., None]], axis=-1)
    solved = lax.linalg.triangular_solve(identity + coupling, right_side, left_side=True, lower=True, unit_diagonal=True)
    val_width = value_t.shape[-2]
    fresh_vals = solved[..., :val_width]
    key_mix = solved[..., val_width:]
    scores = decays * jnp.einsum('...rd,...sd->...rs', query_t, unit_t, precision=FULL_PREC)
    tile_end = cumlog[..., -1]
    carried = unit_t * jnp.exp(tile_end[..., None] - cumlog)[..., None]
    key_eye = jnp.eye(unit_t.shape[-1], dtype=carried.dtype)
    tile_map = jnp.exp(tile_end)[..., None, None] * key_eye - jnp.einsum('...rd,...re->...de', key_mix, carried, precision=FULL_PREC)
    tile_add = jnp.einsum('...rv,...rd->...vd', fresh_vals, carried, precision=FULL_PREC)
    return (fresh_vals, key_mix, scores, cumlog, tile_map, tile_add)

def tile_output(start_state, query_t, key_mix, fresh_vals, scores, cumlog):
    new_vals = fresh_vals - jnp.einsum('...rd,...vd->...rv', key_mix, start_state, precision=FULL_PREC)
    direct_term = jnp.einsum('...vd,...rd->...vr', start_state, query_t * jnp.exp(cumlog)[..., None], precision=FULL_PREC)
    return direct_term + jnp.einsum('...sv,...rs->...vr', new_vals, scores, precision=FULL_PREC)

def head_pass(head_items):
    query_h, unit_h, value_h, rate_h, decay_h = head_items
    tile_count = TOK_DEV // TILE
    query_t = query_h.astype(jnp.float32).reshape(SEQUENCE_COUNT, N_SEQ, tile_count, TILE, DK)
    unit_t = unit_h.reshape(SEQUENCE_COUNT, N_SEQ, tile_count, TILE, DK)
    value_t = value_h.astype(jnp.float32).reshape(SEQUENCE_COUNT, DV, N_SEQ, tile_count, TILE).transpose(0, 2, 3, 1, 4)
    rate_t = rate_h.reshape(SEQUENCE_COUNT, N_SEQ, tile_count, TILE)
    decay_t = decay_h.reshape(SEQUENCE_COUNT, N_SEQ, tile_count, TILE)
    fresh_vals, key_mix, scores, cumlog, tile_map, tile_add = tile_terms(query_t, unit_t, value_t, rate_t, decay_t)

    def advance(carried_pair, inputs):
        state_now, trans_now = carried_pair
        map_now, add_now = inputs
        return ((apply_map(state_now, map_now) + add_now, apply_map(trans_now, map_now)), None)
    initial = (jnp.zeros((SEQUENCE_COUNT, N_SEQ, DV, DK), jnp.float32), jnp.broadcast_to(jnp.eye(DK, dtype=jnp.float32), (SEQUENCE_COUNT, N_SEQ, DK, DK)))
    (block_end, block_map), _ = lax.scan(advance, initial, (jnp.moveaxis(tile_map, 2, 0), jnp.moveaxis(tile_add, 2, 0)))
    moving = block_end
    start_state = jnp.zeros_like(block_end)
    for hop_num in range(WINDOW):
        arrived = jnp.concatenate([jnp.zeros_like(moving[:, :1]), moving[:, :-1]], axis=1)
        start_state = start_state + arrived
        moving = apply_map(arrived, block_map)

    def emit_tile(state_now, inputs):
        query_x, mix_x, fresh_x, scores_x, cum_x, map_x, add_x = inputs
        result = tile_output(state_now, query_x, mix_x, fresh_x, scores_x, cum_x)
        return (apply_map(state_now, map_x) + add_x, result)
    _, tile_outs = lax.scan(emit_tile, start_state, tuple((jnp.moveaxis(item, 2, 0) for item in (query_t, key_mix, fresh_vals, scores, cumlog, tile_map, tile_add))))
    return tile_outs.transpose(1, 3, 2, 0, 4).reshape(SEQUENCE_COUNT, DV, TOKEN_COUNT)

def reference(query, key, value, out_gate, beta, log_decay, lengths, norm_gain):
    position = jnp.arange(TOKEN_COUNT)
    within = position % TOK_DEV
    owner_blk = (position // TOK_DEV).astype(jnp.int32)
    live_mask = (within[None, :] < lengths[:, owner_blk]).astype(jnp.float32)
    key_float = key.astype(jnp.float32)
    unit_key = key_float / jnp.sqrt(lax.optimization_barrier(jnp.sum(key_float * key_float, axis=-1, keepdims=True)) + 1e-06)
    eff_rate = beta * live_mask[:, None, :]
    eff_decay = log_decay * live_mask[:, None, :]
    raw_out = lax.map(head_pass, (jnp.swapaxes(query, 0, 1), jnp.swapaxes(unit_key, 0, 1), jnp.swapaxes(value, 0, 1), jnp.swapaxes(eff_rate, 0, 1), jnp.swapaxes(eff_decay, 0, 1)))
    raw_out = jnp.swapaxes(raw_out, 0, 1)
    mean_sq = lax.optimization_barrier(jnp.mean(raw_out * raw_out, axis=2))
    gated_out = raw_out * lax.rsqrt(mean_sq + 1e-06)[:, :, None, :] * norm_gain[None, None, :, None] * jax.nn.silu(out_gate.astype(jnp.float32)) * live_mask[:, None, None, :]
    return gated_out.astype(jnp.bfloat16)
```

```python
import jax
import jax.numpy as jnp
from jax import lax
from jax.experimental import pallas as pl
from jax.experimental.pallas import tpu as pltpu
from jax.sharding import PartitionSpec as P

WINDOW = 4
F32 = jnp.float32
BF16 = jnp.bfloat16


def dot(left, right):
    return jnp.dot(left, right, preferred_element_type=F32)


def split(full):
    high = full.astype(BF16)
    return high, (full - high.astype(F32)).astype(BF16)


def stack_rows(rows):
    blank = jnp.zeros_like(rows[0])
    return jnp.concatenate(rows + [blank] * (-len(rows) % 8), axis=0)


def state_kernel(
    lengths, key, value, beta, log_decay, end_out, map_out, inv_out, fix_out, decay_out, keys_out, cum_out
):
    seqs, heads, tokens, width = key.shape
    val_width = value.shape[2]
    half = tokens // 2
    pairs = [(b, h) for b in range(seqs) for h in range(heads)]
    lane = lax.broadcasted_iota(jnp.int32, (1, tokens), 1)
    row = lax.broadcasted_iota(jnp.int32, (tokens, tokens), 0)
    col = lax.broadcasted_iota(jnp.int32, (tokens, tokens), 1)
    upto = row <= col
    before = row < col
    eye = (row == col).astype(F32)
    low_row = lax.broadcasted_iota(jnp.int32, (half, half), 0)
    low_col = lax.broadcasted_iota(jnp.int32, (half, half), 1)
    apart = low_row ^ low_col
    low_eye = (low_row == low_col).astype(F32)

    live = [lane < lengths[b, 0] for b, _ in pairs]
    decays = stack_rows([jnp.where(live[i], log_decay[b, pl.ds(h, 1), :], 0.0) for i, (b, h) in enumerate(pairs)])
    ones = upto.astype(BF16)
    part0 = decays.astype(BF16)
    rest = decays - part0.astype(F32)
    part1 = rest.astype(BF16)
    part2 = (rest - part1.astype(F32)).astype(BF16)
    cum = dot(part0, ones) + (dot(part1, ones) + dot(part2, ones))
    cum_out[...] = cum

    keys_t, norms, scaled, weights, cums = [], [], [], [], []
    for i, (b, h) in enumerate(pairs):
        key_t = key[b, h].T
        wide = key_t.astype(F32)
        squares = jnp.sum(wide * wide, axis=0, keepdims=True) + 1e-06
        norm = lax.rsqrt(squares)
        c = cum[i : i + 1]
        rate = beta[b, pl.ds(h, 1), :]
        shift = jnp.where(live[i], c + 0.5 * jnp.log(squares) - jnp.log(rate), 1e30)
        weight = jnp.where(live[i], rate * norm * jnp.exp(c[:, tokens - 1 :] - c), 0.0)
        keys_t.append(key_t)
        norms.append(norm)
        cums.append(c)
        scaled.append(shift)
        weights.append(weight)
    columns = stack_rows(scaled + weights).T
    count = len(pairs)

    couplings, lows = [], []
    for i, (b, h) in enumerate(pairs):
        decay = jnp.exp(jnp.where(upto, cums[i] - columns[:, i : i + 1], -1e30))
        decay_out[i] = decay
        gram = dot(key[b, h], keys_t[i])
        couplings.append(jnp.where(before, gram * decay * norms[i], 0.0))
        for s in (0, half):
            lows.append(couplings[i][s : s + half, s : s + half])

    steps = [jnp.where(apart < 4, low, 0.0).astype(BF16) for low in lows]
    twos = [dot(n, n) for n in steps]
    invs = [low_eye - n.astype(F32) + t - dot(n, t.astype(BF16)) for n, t in zip(steps, twos)]
    size = 4
    while size < half:
        narrow = [x.astype(BF16) for x in invs]
        links = [
            jnp.where((apart >= size) & (apart < 2 * size), low, 0.0).astype(BF16) for low in lows
        ]
        mids = [dot(x, c).astype(BF16) for x, c in zip(narrow, links)]
        invs = [x - dot(m, n) for x, m, n in zip(invs, mids, narrow)]
        size *= 2

    coarse = []
    for i in range(count):
        first, second = invs[2 * i].astype(BF16), invs[2 * i + 1].astype(BF16)
        mid = dot(first, couplings[i][:half, half:].astype(BF16)).astype(BF16)
        corner = -dot(mid, second)
        coarse.append(
            jnp.concatenate(
                [
                    jnp.concatenate([first, corner.astype(BF16)], axis=1),
                    jnp.concatenate([jnp.zeros_like(first), second], axis=1),
                ],
                axis=0,
            )
        )
    fixes = []
    for i in range(count):
        high, low = split(couplings[i])
        left = (eye - coarse[i].astype(F32)) - (dot(high, coarse[i]) + dot(low, coarse[i]))
        fixes.append(dot(coarse[i], left.astype(BF16)).astype(BF16))
    for i, (b, h) in enumerate(pairs):
        inv_out[i] = coarse[i]
        fix_out[i] = fixes[i]
        high, low = split(key[b, h].astype(F32) * columns[:, count + i : count + i + 1])
        mixed = dot(coarse[i], high) + (dot(coarse[i], low) + dot(fixes[i], high))
        mixed_high, mixed_low = split(mixed)
        key_high, key_low = split(keys_t[i].astype(F32) * (jnp.exp(cums[i]) * norms[i]))
        stacked = jnp.concatenate([value[b, h], key_high, key_low], axis=0)
        keys_out[i] = stacked
        main = dot(stacked, mixed_high)
        extra = dot(stacked[: val_width + width], mixed_low)
        end_out[b, h] = main[:val_width] + extra[:val_width]
        taken = main[val_width : val_width + width] + (main[val_width + width :] + extra[val_width:])
        whole = jnp.exp(cums[i][:, tokens - 1 :])
        map_out[b, h] = whole * eye[:width, :width] - taken


def output_kernel(query, key, inv, fix, decay, keys, cum, own_out, carry_out):
    seqs, heads, tokens, width = query.shape
    val_width = own_out.shape[2]
    for b in range(seqs):
        for h in range(heads):
            i = b * heads + h
            query_t = query[b, h].T
            scores = dot(key[b, h], query_t) * decay[i]
            high, low = split(scores)
            mixed = dot(inv[i], high) + (dot(inv[i], low) + dot(fix[i], high))
            mixed_high, mixed_low = split(mixed)
            stacked = keys[i]
            main = dot(stacked, mixed_high)
            extra = dot(stacked[: val_width + width], mixed_low)
            own_out[b, h] = main[:val_width] + extra[:val_width]
            taken = main[val_width : val_width + width] + (main[val_width + width :] + extra[val_width:])
            carry_out[b, h] = query_t.astype(F32) * jnp.exp(cum[i : i + 1]) - taken


def raw_kernel(own, carry, state, raw_out, square_out):
    seqs, heads = own.shape[:2]
    rows = []
    for b in range(seqs):
        for h in range(heads):
            raw = own[b, h] + jnp.dot(
                state[b, h], carry[b, h], precision=lax.Precision.HIGH, preferred_element_type=F32
            )
            raw_out[b, h] = raw
            rows.append(jnp.sum(raw * raw, axis=0, keepdims=True))
    square_out[...] = stack_rows(rows)


def gate_kernel(lengths, raw, squares, gate, gain, out):
    seqs, heads, val_width, tokens = raw.shape
    total = jnp.sum(squares[...], axis=0)
    scale = lax.rsqrt(total / (val_width * squares.shape[0]) + 1e-06)
    lane = lax.broadcasted_iota(jnp.int32, (1, tokens), 1)
    for b in range(seqs):
        live = lane < lengths[b, 0]
        for h in range(heads):
            i = b * heads + h
            opened = gate[b, h].astype(F32)
            opened = opened / (1.0 + jnp.exp(-opened))
            factor = jnp.where(live, scale[i : i + 1], 0.0)
            out[b, h] = (raw[b, h] * factor * (gain[...] * opened)).astype(BF16)


def vmem(count):
    return [pl.BlockSpec(memory_space=pltpu.VMEM)] * count


def call(body, outs, *operands, scalars=0):
    return pl.pallas_call(
        body,
        out_shape=outs,
        in_specs=[pl.BlockSpec(memory_space=pltpu.SMEM)] * scalars + vmem(len(operands) - scalars),
        out_specs=jax.tree.map(lambda _: pl.BlockSpec(memory_space=pltpu.VMEM), outs),
        compiler_params=pltpu.CompilerParams(vmem_limit_bytes=60 * 1024 * 1024),
    )(*operands)


def local(query, key, value, out_gate, beta, log_decay, lengths, norm_gain):
    seqs, heads, tokens, width = query.shape
    val_width = value.shape[2]
    count = seqs * heads
    shape = jax.ShapeDtypeStruct
    block_end, block_map, inverse, fix, decay, keys, cum = call(
        state_kernel,
        (
            shape((seqs, heads, val_width, width), F32),
            shape((seqs, heads, width, width), F32),
            shape((count, tokens, tokens), BF16),
            shape((count, tokens, tokens), BF16),
            shape((count, tokens, tokens), F32),
            shape((count, val_width + 2 * width, tokens), BF16),
            shape((count + -count % 8, tokens), F32),
        ),
        lengths,
        key,
        value,
        beta,
        log_decay,
        scalars=1,
    )
    devices = lax.axis_size("seq")
    moving = block_end
    state = None
    for hop in range(1, WINDOW + 1):
        moving = lax.ppermute(moving, "seq", [(s, s + 1) for s in range(hop - 1, devices - 1)])
        state = moving if state is None else state + moving
        if hop < WINDOW:
            moving = jnp.matmul(moving, block_map, precision=lax.Precision.HIGH)
    own, carry = call(
        output_kernel,
        (
            shape((seqs, heads, val_width, tokens), F32),
            shape((seqs, heads, width, tokens), F32),
        ),
        query,
        key,
        inverse,
        fix,
        decay,
        keys,
        cum,
    )
    raw, squares = call(
        raw_kernel,
        (
            shape((seqs, heads, val_width, tokens), F32),
            shape((count + -count % 8, tokens), F32),
        ),
        own,
        carry,
        state,
    )
    squares = lax.all_gather(squares, "dim")
    return call(
        gate_kernel,
        shape((seqs, heads, val_width, tokens), BF16),
        lengths,
        raw,
        squares,
        out_gate,
        norm_gain[:, None],
        scalars=1,
    )


def solution(mesh):
    in_specs = (
        P("groups", "head", "seq", None),
        P("groups", "head", "seq", None),
        P("groups", "head", "dim", "seq"),
        P("groups", "head", "dim", "seq"),
        P("groups", "head", "seq"),
        P("groups", "head", "seq"),
        P("groups", "seq"),
        P("dim"),
    )
    out_specs = P("groups", "head", "dim", "seq")
    return jax.shard_map(local, mesh=mesh, in_specs=in_specs, out_specs=out_specs, check_vma=False)
```

```python
import jax
import jax.numpy as jnp
from jax import lax
from jax.experimental import pallas as pl
from jax.experimental.pallas import tpu as pltpu
from jax.sharding import PartitionSpec as P

WINDOW = 4
F32 = jnp.float32
BF16 = jnp.bfloat16


def dot(left, right):
    return jnp.dot(left, right, preferred_element_type=F32)


def split(full):
    high = full.astype(BF16)
    return high, (full - high.astype(F32)).astype(BF16)


def stack_rows(rows):
    blank = jnp.zeros_like(rows[0])
    return jnp.concatenate(rows + [blank] * (-len(rows) % 8), axis=0)


def state_kernel(
    lengths_in,
    key_in,
    value_in,
    beta_in,
    log_decay_in,
    query_in,
    gate_in,
    gain_in,
    end_out,
    mix_out,
    inv_out,
    fix_out,
    decay_out,
    keys_out,
    cum_out,
    live_out,
    key,
    query_out,
    gate_out,
    gain_out,
    value,
    lengths,
    high_ref,
    low_ref,
    beta,
    log_decay,
    sems,
):
    sources = [lengths_in, log_decay_in, beta_in, key_in, value_in, query_in, gate_in, gain_in]
    places = [lengths, log_decay, beta, key, value, query_out, gate_out, gain_out]
    copies = [pltpu.make_async_copy(s, p, sems.at[n]) for n, (s, p) in enumerate(zip(sources, places))]
    for copy in copies:
        copy.start()
    seqs, heads, tokens, width = key.shape
    val_width = value.shape[2]
    half = tokens // 2
    pairs = [(b, h) for b in range(seqs) for h in range(heads)]
    count = len(pairs)
    lane = lax.broadcasted_iota(jnp.int32, (1, tokens), 1)
    row = lax.broadcasted_iota(jnp.int32, (tokens, tokens), 0)
    col = lax.broadcasted_iota(jnp.int32, (tokens, tokens), 1)
    ones = (row <= col).astype(BF16)
    low_row = lax.broadcasted_iota(jnp.int32, (half, half), 0)
    low_col = lax.broadcasted_iota(jnp.int32, (half, half), 1)
    apart = low_row ^ low_col
    low_eye = (low_row == low_col).astype(F32)
    wide_eye = jnp.concatenate([low_eye, jnp.zeros_like(low_eye)], axis=1)
    masks = [(apart < 4).astype(BF16)]
    size = 4
    while size < half:
        masks.append(((apart >= size) & (apart < 2 * size)).astype(BF16))
        size *= 2

    for copy in copies[:2]:
        copy.wait()
    live = [lane < lengths[0, b] for b, _ in pairs]
    live_out[...] = stack_rows([mask.astype(F32) for mask in live])
    decays = stack_rows([jnp.where(live[i], log_decay[b, pl.ds(h, 1), :], 0.0) for i, (b, h) in enumerate(pairs)])
    part0 = decays.astype(BF16)
    rest = decays - part0.astype(F32)
    part1 = rest.astype(BF16)
    part2 = (rest - part1.astype(F32)).astype(BF16)
    cum = dot(part0, ones) + (dot(part1, ones) + dot(part2, ones))
    cum_out[...] = cum

    for copy in copies[2:4]:
        copy.wait()
    keys_t, norms, shifts, weights, cums = [], [], [], [], []
    for i, (b, h) in enumerate(pairs):
        key_t = key[b, h].T
        wide = key_t.astype(F32)
        squares = jnp.sum(wide * wide, axis=0, keepdims=True) + 1e-06
        norm = lax.rsqrt(squares)
        c = cum[i : i + 1]
        rate = beta[b, pl.ds(h, 1), :]
        keys_t.append(key_t)
        norms.append(norm)
        cums.append(c)
        shifts.append(jnp.where(live[i], c + 0.5 * jnp.log(squares) - jnp.log(rate), 1e30))
        weights.append(jnp.where(live[i], rate * norm * jnp.exp(c[:, tokens - 1 :] - c), 0.0))
    columns = stack_rows(shifts + weights).T

    grams = [
        [
            dot(key[b, h, :half], keys_t[i]),
            dot(key[b, h, half:], keys_t[i][:, half:]),
        ]
        for i, (b, h) in enumerate(pairs)
    ]
    for i in range(count):
        shift = columns[:, i : i + 1]
        for r, c in ((0, 0), (0, half), (half, half)):
            gap = cums[i][:, c : c + half] - shift[r : r + half]
            if r == c:
                gap = jnp.where(low_row <= low_col, gap, -1e30)
            decay = jnp.exp(gap)
            decay_out[i, r : r + half, c : c + half] = decay
            gram = grams[i][1] if r else grams[i][0][:, c : c + half]
            link = gram * decay * norms[i][:, c : c + half]
            if r == c:
                link = jnp.where(low_row < low_col, link, 0.0)
            high, low = split(link)
            high_ref[i, r : r + half, c : c + half] = high
            low_ref[i, r : r + half, c : c + half] = low
        high_ref[i, half:, :half] = jnp.zeros((half, half), BF16)
        low_ref[i, half:, :half] = jnp.zeros((half, half), BF16)

    for copy in copies[4:]:
        copy.wait()
    members = range(count)
    blocks = [(i, s) for i in members for s in (0, half)]
    steps = [high_ref[i, s : s + half, s : s + half] * masks[0] for i, s in blocks]
    twos = [dot(n, n) for n in steps]
    invs = [(low_eye - n.astype(F32) + t - dot(n, t.astype(BF16))).astype(BF16) for n, t in zip(steps, twos)]
    for mask in masks[1:]:
        mids = [
            dot(x, high_ref[i, s : s + half, s : s + half] * mask).astype(BF16) for x, (i, s) in zip(invs, blocks)
        ]
        invs = [x - dot(m, x).astype(BF16) for x, m in zip(invs, mids)]
    mids = [dot(invs[2 * i], high_ref[i, :half, half:]).astype(BF16) for i in members]
    corners = [-dot(mid, invs[2 * i + 1]).astype(BF16) for i, mid in enumerate(mids)]
    for i in members:
        inv_out[i, :half, :half] = invs[2 * i]
        inv_out[i, :half, half:] = corners[i]
        inv_out[i, half:, :half] = jnp.zeros_like(corners[i])
        inv_out[i, half:, half:] = invs[2 * i + 1]
    sides = [split(key[pairs[i]].astype(F32) * columns[:, count + i : count + i + 1]) for i in members]
    tops = [
        dot(
            jnp.concatenate([inv_out[i, :half], inv_out[i, :half]], axis=1),
            jnp.concatenate([high_ref[i], low_ref[i]], axis=0),
        )
        for i in members
    ]
    bottoms = [
        dot(
            jnp.concatenate([invs[2 * i + 1], invs[2 * i + 1]], axis=1),
            jnp.concatenate([high_ref[i, half:, half:], low_ref[i, half:, half:]], axis=0),
        )
        for i in members
    ]
    mixes = [dot(inv_out[i], jnp.concatenate(sides[i], axis=1)) for i in members]
    for i in members:
        fix_out[i, :half] = (wide_eye - inv_out[i, :half].astype(F32) - tops[i]).astype(BF16)
        fix_out[i, half:, :half] = jnp.zeros((half, half), BF16)
        fix_out[i, half:, half:] = (low_eye - invs[2 * i + 1].astype(F32) - bottoms[i]).astype(BF16)
    mixes = [mixed[:, :width] + mixed[:, width:] for mixed in mixes]
    parts = [split(mixed + dot(fix_out[i], mixed.astype(BF16))) for i, mixed in enumerate(mixes)]
    for i, (high, low) in enumerate(parts):
        end_out[pairs[i]] = from_values_narrow(value[pairs[i]], high, low)
        mix_out[i, 0] = high
        mix_out[i, 1] = low
    for i in members:
        key_high, key_low = split(keys_t[i].astype(F32) * (jnp.exp(cums[i]) * norms[i]))
        keys_out[i, 0] = key_high
        keys_out[i, 1] = key_low


def from_values(value, high, low):
    return dot(jnp.concatenate([value, value], axis=1), jnp.concatenate([high, low], axis=0))


def from_values_narrow(value, high, low):
    both = dot(value, jnp.concatenate([high, low], axis=1))
    return both[:, : high.shape[1]] + both[:, high.shape[1] :]


def from_keys(key_high, key_low, high, low):
    return dot(
        jnp.concatenate([key_high, key_low, key_high], axis=1), jnp.concatenate([high, high, low], axis=0)
    )


def output_kernel(query, key, value, mix, inv, fix, decay, keys, cum, own_out, carry_out, map_out):
    seqs, heads, tokens, width = query.shape
    half = tokens // 2
    pairs = [(b, h) for b in range(seqs) for h in range(heads)]
    queries = [query[pair].T for pair in pairs]
    fixes = [dot(fix[i], inv[i]) for i in range(len(pairs))]
    tops = [dot(key[b, h, :half], query_t) for (b, h), query_t in zip(pairs, queries)]
    bottoms = [dot(key[b, h, half:], query_t[:, half:]) for (b, h), query_t in zip(pairs, queries)]
    parts = []
    for i, (top, bottom) in enumerate(zip(tops, bottoms)):
        bottom = bottom * decay[i, half:, half:]
        bottom = jnp.concatenate([jnp.zeros_like(bottom), bottom], axis=1)
        parts.append(split(jnp.concatenate([top * decay[i, :half], bottom], axis=0)))
    mixes = [
        dot(
            jnp.concatenate([inv[i], inv[i], fixes[i].astype(BF16)], axis=1),
            jnp.concatenate([high, low, high], axis=0),
        )
        for i, (high, low) in enumerate(parts)
    ]
    eye = (
        lax.broadcasted_iota(jnp.int32, (width, width), 0) == lax.broadcasted_iota(jnp.int32, (width, width), 1)
    ).astype(F32)
    for i, pair in enumerate(pairs):
        whole = jnp.exp(cum[i : i + 1, tokens - 1 :])
        both = from_values_narrow(keys[i, 0], mix[i, 0], mix[i, 1])
        map_out[pair] = whole * eye - (both + dot(keys[i, 1], mix[i, 0]))
    parts = [split(mixed) for mixed in mixes]
    for i, (high, low) in enumerate(parts):
        own_out[pairs[i]] = from_values(value[pairs[i]], high, low)
    for i, (high, low) in enumerate(parts):
        taken = from_keys(keys[i, 0], keys[i, 1], high, low)
        carry_out[pairs[i]] = queries[i].astype(F32) * jnp.exp(cum[i : i + 1]) - taken


def raw_kernel(own, carry, *rest):
    *states, raw_out, square_out = rest
    seqs, heads = own.shape[:2]
    rows = []
    for b in range(seqs):
        for h in range(heads):
            state = states[0][b, h]
            for arrived in states[1:]:
                state = state + arrived[b, h]
            raw = own[b, h] + jnp.dot(
                state, carry[b, h], precision=lax.Precision.HIGH, preferred_element_type=F32
            )
            raw_out[b, h] = raw
            rows.append(jnp.sum(raw * raw, axis=0, keepdims=True))
    square_out[...] = stack_rows(rows)


def gate_kernel(raw, squares, gate, gain, live, out):
    seqs, heads, val_width, tokens = raw.shape
    total = jnp.sum(squares[...], axis=0)
    scale = lax.rsqrt(total / (val_width * squares.shape[0]) + 1e-06)
    gains = jnp.broadcast_to(gain[...], (8, val_width)).T[:, :1]
    scale = scale * live[...]
    for b in range(seqs):
        for h in range(heads):
            i = b * heads + h
            opened = gate[b, h].astype(F32)
            opened = opened / (1.0 + jnp.exp(-opened))
            out[b, h] = (raw[b, h] * scale[i : i + 1] * (gains * opened)).astype(BF16)


VMEM = pl.BlockSpec(memory_space=pltpu.VMEM)


def call(body, outs, *operands, space=VMEM, scratch=()):
    return pl.pallas_call(
        body,
        out_shape=outs,
        in_specs=[space] * len(operands),
        out_specs=jax.tree.map(lambda _: VMEM, outs),
        scratch_shapes=scratch,
        compiler_params=pltpu.CompilerParams(vmem_limit_bytes=16 * 1024 * 1024),
    )(*operands)


def local(query, key, value, out_gate, beta, log_decay, lengths, norm_gain):
    seqs, heads, tokens, width = query.shape
    val_width = value.shape[2]
    count = seqs * heads
    shape = jax.ShapeDtypeStruct
    rows = shape((count + -count % 8, tokens), F32)
    lengths = lengths.T
    norm_gain = norm_gain[None, :]
    block_end, mix, inverse, fix, decay, keys, cum, live, key, query, out_gate, norm_gain, value = call(
        state_kernel,
        (
            shape((seqs, heads, val_width, width), F32),
            shape((count, 2, tokens, width), BF16),
            shape((count, tokens, tokens), BF16),
            shape((count, tokens, tokens), BF16),
            shape((count, tokens, tokens), F32),
            shape((count, 2, width, tokens), BF16),
            rows,
            rows,
            shape(key.shape, BF16),
            shape(query.shape, BF16),
            shape(out_gate.shape, BF16),
            shape(norm_gain.shape, F32),
            shape(value.shape, BF16),
        ),
        *[
            pltpu.with_memory_space_constraint(array, pltpu.HBM)
            for array in (lengths, key, value, beta, log_decay, query, out_gate, norm_gain)
        ],
        space=pl.BlockSpec(memory_space=pltpu.HBM),
        scratch=[
            pltpu.SMEM(lengths.shape, jnp.int32),
            pltpu.VMEM((count, tokens, tokens), BF16),
            pltpu.VMEM((count, tokens, tokens), BF16),
            pltpu.VMEM(beta.shape, F32),
            pltpu.VMEM(log_decay.shape, F32),
            pltpu.SemaphoreType.DMA((8,)),
        ],
    )
    steps = lax.axis_size("seq") - 1
    arrived = [lax.ppermute(block_end, "seq", [(s, s + 1) for s in range(steps)])]
    own, carry, block_map = call(
        output_kernel,
        (
            shape((seqs, heads, val_width, tokens), F32),
            shape((seqs, heads, width, tokens), F32),
            shape((seqs, heads, width, width), F32),
        ),
        query,
        key,
        value,
        mix,
        inverse,
        fix,
        decay,
        keys,
        cum,
    )
    for hop in range(1, WINDOW):
        moving = jnp.matmul(arrived[-1], block_map, precision=lax.Precision.HIGH)
        arrived.append(lax.ppermute(moving, "seq", [(s, s + 1) for s in range(hop, steps)]))
    raw, squares = call(
        raw_kernel,
        (shape((seqs, heads, val_width, tokens), F32), rows),
        own,
        carry,
        *arrived,
    )
    squares = lax.all_gather(squares, "dim")
    return call(
        gate_kernel,
        shape((seqs, heads, val_width, tokens), BF16),
        raw,
        squares,
        out_gate,
        norm_gain,
        live,
    )


def solution(mesh):
    in_specs = (
        P("groups", "head", "seq", None),
        P("groups", "head", "seq", None),
        P("groups", "head", "dim", "seq"),
        P("groups", "head", "dim", "seq"),
        P("groups", "head", "seq"),
        P("groups", "head", "seq"),
        P("groups", "seq"),
        P("dim"),
    )
    out_specs = P("groups", "head", "dim", "seq")
    return jax.shard_map(local, mesh=mesh, in_specs=in_specs, out_specs=out_specs, check_vma=False)
```

```python
import jax
import jax.numpy as jnp
from jax import lax
from jax.experimental import pallas as pl
from jax.experimental.pallas import tpu as pltpu
from jax.sharding import PartitionSpec as P


F32 = jnp.float32
BF16 = jnp.bfloat16


def dot(left, right):
    return jnp.dot(left, right, preferred_element_type=F32)


def exact_dot(left, right):
    return jnp.dot(left, right, precision=lax.Precision.HIGH, preferred_element_type=F32)


def apply_map(left, right):
    return jnp.matmul(left, right, precision=lax.Precision.HIGH)


def passed(value, distance, first, last):
    return lax.ppermute(value, "seq", [(s, s + distance) for s in range(first, last)])


def split(full):
    high = full.astype(BF16)
    return high, (full - high.astype(F32)).astype(BF16)


def stack_rows(rows):
    blank = jnp.zeros_like(rows[0])
    return jnp.concatenate(rows + [blank] * (-len(rows) % 8), axis=0)


def state_kernel(
    lengths_in,
    key_in,
    value_in,
    beta_in,
    log_decay_in,
    query_in,
    gate_in,
    gain_in,
    end_out,
    mix_out,
    inv_out,
    fix_out,
    decay_out,
    keys_out,
    cum_out,
    live_out,
    key,
    query_out,
    gate_out,
    gain_out,
    value,
    lengths,
    high_ref,
    low_ref,
    beta,
    log_decay,
    sems,
):
    sources = [lengths_in, log_decay_in, beta_in, key_in, value_in, query_in, gate_in, gain_in]
    places = [lengths, log_decay, beta, key, value, query_out, gate_out, gain_out]
    copies = [pltpu.make_async_copy(s, p, sems.at[n]) for n, (s, p) in enumerate(zip(sources, places))]
    for copy in copies:
        copy.start()
    seqs, heads, tokens, width = key.shape
    half = tokens // 2
    pairs = [(b, h) for b in range(seqs) for h in range(heads)]
    count = len(pairs)
    lane = lax.broadcasted_iota(jnp.int32, (1, tokens), 1)
    row = lax.broadcasted_iota(jnp.int32, (tokens, tokens), 0)
    col = lax.broadcasted_iota(jnp.int32, (tokens, tokens), 1)
    ones = (row <= col).astype(BF16)
    low_row = lax.broadcasted_iota(jnp.int32, (half, half), 0)
    low_col = lax.broadcasted_iota(jnp.int32, (half, half), 1)
    apart = low_row ^ low_col
    low_eye = (low_row == low_col).astype(F32)
    wide_eye = jnp.concatenate([low_eye, jnp.zeros_like(low_eye)], axis=1)
    masks = [(apart < 4).astype(BF16)]
    size = 4
    while size < half:
        masks.append(((apart >= size) & (apart < 2 * size)).astype(BF16))
        size *= 2

    for copy in copies[:2]:
        copy.wait()
    live = [lane < lengths[0, b] for b, _ in pairs]
    live_out[...] = stack_rows([mask.astype(F32) for mask in live])
    decays = stack_rows([jnp.where(live[i], log_decay[b, pl.ds(h, 1), :], 0.0) for i, (b, h) in enumerate(pairs)])
    part0 = decays.astype(BF16)
    rest = decays - part0.astype(F32)
    part1 = rest.astype(BF16)
    part2 = (rest - part1.astype(F32)).astype(BF16)
    cum = dot(part0, ones) + (dot(part1, ones) + dot(part2, ones))
    cum_out[...] = cum

    for copy in copies[2:4]:
        copy.wait()
    keys_t, norms, shifts, weights, cums = [], [], [], [], []
    for i, (b, h) in enumerate(pairs):
        key_t = key[b, h].T
        wide = key_t.astype(F32)
        squares = jnp.sum(wide * wide, axis=0, keepdims=True) + 1e-06
        norm = lax.rsqrt(squares)
        c = cum[i : i + 1]
        rate = beta[b, pl.ds(h, 1), :]
        keys_t.append(key_t)
        norms.append(norm)
        cums.append(c)
        shifts.append(jnp.where(live[i], c + 0.5 * jnp.log(squares) - jnp.log(rate), 1e30))
        weights.append(jnp.where(live[i], rate * norm * jnp.exp(c[:, tokens - 1 :] - c), 0.0))
    columns = stack_rows(shifts + weights).T

    grams = [
        [
            dot(key[b, h, :half], keys_t[i]),
            dot(key[b, h, half:], keys_t[i][:, half:]),
        ]
        for i, (b, h) in enumerate(pairs)
    ]
    for i in range(count):
        shift = columns[:, i : i + 1]
        for r, c in ((0, 0), (0, half), (half, half)):
            gap = cums[i][:, c : c + half] - shift[r : r + half]
            if r == c:
                gap = jnp.where(low_row <= low_col, gap, -1e30)
            decay = jnp.exp(gap)
            decay_out[i, r : r + half, c : c + half] = decay
            gram = grams[i][1] if r else grams[i][0][:, c : c + half]
            link = gram * decay * norms[i][:, c : c + half]
            if r == c:
                link = jnp.where(low_row < low_col, link, 0.0)
            high, low = split(link)
            high_ref[i, r : r + half, c : c + half] = high
            low_ref[i, r : r + half, c : c + half] = low
        high_ref[i, half:, :half] = jnp.zeros((half, half), BF16)
        low_ref[i, half:, :half] = jnp.zeros((half, half), BF16)

    for copy in copies[4:]:
        copy.wait()
    members = range(count)
    blocks = [(i, s) for i in members for s in (0, half)]
    steps = [high_ref[i, s : s + half, s : s + half] * masks[0] for i, s in blocks]
    twos = [dot(n, n) for n in steps]
    invs = [(low_eye - n.astype(F32) + t - dot(n, t.astype(BF16))).astype(BF16) for n, t in zip(steps, twos)]
    size = 4
    for mask in masks[1:]:
        links = [high_ref[i, s : s + half, s : s + half] * mask for i, s in blocks]
        if size < 16:
            mids = [dot(x, link).astype(BF16) for x, link in zip(invs, links)]
            invs = [x - dot(m, x).astype(BF16) for x, m in zip(invs, mids)]
        else:
            uppers = [jnp.concatenate([x[k : k + size] for k in range(0, half, 2 * size)], axis=0) for x in invs]
            mids = [dot(u, link).astype(BF16) for u, link in zip(uppers, links)]
            uppers = [u - dot(m, x).astype(BF16) for u, m, x in zip(uppers, mids, invs)]
            invs = [
                jnp.concatenate(
                    [
                        piece
                        for k in range(0, half, 2 * size)
                        for piece in (u[k // 2 : k // 2 + size], x[k + size : k + 2 * size])
                    ],
                    axis=0,
                )
                for u, x in zip(uppers, invs)
            ]
        size *= 2
    mids = [dot(invs[2 * i], high_ref[i, :half, half:]).astype(BF16) for i in members]
    corners = [-dot(mid, invs[2 * i + 1]).astype(BF16) for i, mid in enumerate(mids)]
    for i in members:
        inv_out[i, :half, :half] = invs[2 * i]
        inv_out[i, :half, half:] = corners[i]
        inv_out[i, half:, :half] = jnp.zeros_like(corners[i])
        inv_out[i, half:, half:] = invs[2 * i + 1]
    sides = [split(key[pairs[i]].astype(F32) * columns[:, count + i : count + i + 1]) for i in members]
    tops = [
        dot(
            jnp.concatenate([inv_out[i, :half], inv_out[i, :half]], axis=1),
            jnp.concatenate([high_ref[i], low_ref[i]], axis=0),
        )
        for i in members
    ]
    bottoms = [
        dot(
            jnp.concatenate([invs[2 * i + 1], invs[2 * i + 1]], axis=1),
            jnp.concatenate([high_ref[i, half:, half:], low_ref[i, half:, half:]], axis=0),
        )
        for i in members
    ]
    mixes = [dot(inv_out[i], jnp.concatenate(sides[i], axis=1)) for i in members]
    for i in members:
        fix_out[i, :half] = (wide_eye - inv_out[i, :half].astype(F32) - tops[i]).astype(BF16)
        fix_out[i, half:, :half] = jnp.zeros((half, half), BF16)
        fix_out[i, half:, half:] = (low_eye - invs[2 * i + 1].astype(F32) - bottoms[i]).astype(BF16)
    mixes = [mixed[:, :width] + mixed[:, width:] for mixed in mixes]
    parts = [split(mixed + dot(fix_out[i], mixed.astype(BF16))) for i, mixed in enumerate(mixes)]
    for i, (high, low) in enumerate(parts):
        end_out[pairs[i]] = from_values_narrow(value[pairs[i]], high, low)
        mix_out[i, 0] = high
        mix_out[i, 1] = low
    for i in members:
        key_high, key_low = split(keys_t[i].astype(F32) * (jnp.exp(cums[i]) * norms[i]))
        keys_out[i, 0] = key_high
        keys_out[i, 1] = key_low


def from_values(value, high, low):
    return dot(jnp.concatenate([value, value], axis=1), jnp.concatenate([high, low], axis=0))


def from_values_narrow(value, high, low):
    both = dot(value, jnp.concatenate([high, low], axis=1))
    return both[:, : high.shape[1]] + both[:, high.shape[1] :]


def from_keys(key_high, key_low, high, low):
    return dot(
        jnp.concatenate([key_high, key_low, key_high], axis=1), jnp.concatenate([high, high, low], axis=0)
    )


def output_kernel(
    query, key, value, mix, inv, fix, decay, keys, cum, gate, gain, live, own_out, carry_out, map_out, factor_out
):
    seqs, heads, tokens, width = query.shape
    half = tokens // 2
    pairs = [(b, h) for b in range(seqs) for h in range(heads)]
    queries = [query[pair].T for pair in pairs]
    fixes = [dot(fix[i], inv[i]) for i in range(len(pairs))]
    tops = [dot(key[b, h, :half], query_t) for (b, h), query_t in zip(pairs, queries)]
    bottoms = [dot(key[b, h, half:], query_t[:, half:]) for (b, h), query_t in zip(pairs, queries)]
    parts = []
    for i, (top, bottom) in enumerate(zip(tops, bottoms)):
        bottom = bottom * decay[i, half:, half:]
        bottom = jnp.concatenate([jnp.zeros_like(bottom), bottom], axis=1)
        parts.append(split(jnp.concatenate([top * decay[i, :half], bottom], axis=0)))
    mixes = [
        dot(
            jnp.concatenate([inv[i], inv[i], fixes[i].astype(BF16)], axis=1),
            jnp.concatenate([high, low, high], axis=0),
        )
        for i, (high, low) in enumerate(parts)
    ]
    eye = (
        lax.broadcasted_iota(jnp.int32, (width, width), 0) == lax.broadcasted_iota(jnp.int32, (width, width), 1)
    ).astype(F32)
    for i, pair in enumerate(pairs):
        whole = jnp.exp(cum[i : i + 1, tokens - 1 :])
        both = from_values_narrow(keys[i, 0], mix[i, 0], mix[i, 1])
        map_out[pair] = whole * eye - (both + dot(keys[i, 1], mix[i, 0]))
    gains = jnp.broadcast_to(gain[...], (8, gain.shape[1])).T[:, :1]
    for i, pair in enumerate(pairs):
        opened = gate[pair].astype(F32)
        factor_out[pair] = gains * (opened / (1.0 + jnp.exp(-opened))) * live[i : i + 1]
    parts = [split(mixed) for mixed in mixes]
    for i, (high, low) in enumerate(parts):
        own_out[pairs[i]] = from_values(value[pairs[i]], high, low)
    for i, (high, low) in enumerate(parts):
        taken = from_keys(keys[i, 0], keys[i, 1], high, low)
        carry_out[pairs[i]] = queries[i].astype(F32) * jnp.exp(cum[i : i + 1]) - taken


def raw_kernel(own, carry, near, next_near, far, product, raw_out, square_out):
    seqs, heads = own.shape[:2]
    pairs = [(b, h) for b in range(seqs) for h in range(heads)]
    states = [(near[pair] + next_near[pair]) + exact_dot(far[pair], product[pair]) for pair in pairs]
    raws = [own[pair] + exact_dot(state, carry[pair]) for pair, state in zip(pairs, states)]
    for pair, raw in zip(pairs, raws):
        raw_out[pair] = raw
    square_out[...] = stack_rows([jnp.sum(raw * raw, axis=0, keepdims=True) for raw in raws])


def gate_kernel(raw, squares, factor, out):
    seqs, heads, val_width, _ = raw.shape
    total = jnp.sum(squares[...], axis=0)
    scale = lax.rsqrt(total / (val_width * squares.shape[0]) + 1e-06)
    for b in range(seqs):
        for h in range(heads):
            i = b * heads + h
            out[b, h] = (raw[b, h] * scale[i : i + 1] * factor[b, h]).astype(BF16)


VMEM = pl.BlockSpec(memory_space=pltpu.VMEM)


def call(body, outs, *operands, space=VMEM, scratch=()):
    return pl.pallas_call(
        body,
        out_shape=outs,
        in_specs=[space] * len(operands),
        out_specs=jax.tree.map(lambda _: VMEM, outs),
        scratch_shapes=scratch,
        compiler_params=pltpu.CompilerParams(vmem_limit_bytes=16 * 1024 * 1024),
    )(*operands)


def local(query, key, value, out_gate, beta, log_decay, lengths, norm_gain):
    seqs, heads, tokens, width = query.shape
    val_width = value.shape[2]
    count = seqs * heads
    shape = jax.ShapeDtypeStruct
    rows = shape((count + -count % 8, tokens), F32)
    lengths = lengths.T
    norm_gain = norm_gain[None, :]
    block_end, mix, inverse, fix, decay, keys, cum, live, key, query, out_gate, norm_gain, value = call(
        state_kernel,
        (
            shape((seqs, heads, val_width, width), F32),
            shape((count, 2, tokens, width), BF16),
            shape((count, tokens, tokens), BF16),
            shape((count, tokens, tokens), BF16),
            shape((count, tokens, tokens), F32),
            shape((count, 2, width, tokens), BF16),
            rows,
            rows,
            shape(key.shape, BF16),
            shape(query.shape, BF16),
            shape(out_gate.shape, BF16),
            shape(norm_gain.shape, F32),
            shape(value.shape, BF16),
        ),
        *[
            pltpu.with_memory_space_constraint(array, pltpu.HBM)
            for array in (lengths, key, value, beta, log_decay, query, out_gate, norm_gain)
        ],
        space=pl.BlockSpec(memory_space=pltpu.HBM),
        scratch=[
            pltpu.SMEM(lengths.shape, jnp.int32),
            pltpu.VMEM((count, tokens, tokens), BF16),
            pltpu.VMEM((count, tokens, tokens), BF16),
            pltpu.VMEM(beta.shape, F32),
            pltpu.VMEM(log_decay.shape, F32),
            pltpu.SemaphoreType.DMA((8,)),
        ],
    )
    steps = lax.axis_size("seq")
    near = passed(block_end, 1, 0, steps - 1)
    own, carry, block_map, factor = call(
        output_kernel,
        (
            shape((seqs, heads, val_width, tokens), F32),
            shape((seqs, heads, width, tokens), F32),
            shape((seqs, heads, width, width), F32),
            shape((seqs, heads, val_width, tokens), F32),
        ),
        query,
        key,
        value,
        mix,
        inverse,
        fix,
        decay,
        keys,
        cum,
        out_gate,
        norm_gain,
        live,
    )
    moved = apply_map(near, block_map)
    far = passed(block_end + moved, 3, 0, steps - 3)
    next_near = passed(moved, 1, 1, steps - 1)
    earlier = passed(block_map, 1, 1, steps - 2)
    product = passed(apply_map(earlier, block_map), 1, 2, steps - 1)
    raw, squares = call(
        raw_kernel,
        (shape((seqs, heads, val_width, tokens), F32), rows),
        own,
        carry,
        near,
        next_near,
        far,
        product,
    )
    squares = lax.all_gather(squares, "dim")
    return call(
        gate_kernel,
        shape((seqs, heads, val_width, tokens), BF16),
        raw,
        squares,
        factor,
    )


def solution(mesh):
    in_specs = (
        P("groups", "head", "seq", None),
        P("groups", "head", "seq", None),
        P("groups", "head", "dim", "seq"),
        P("groups", "head", "dim", "seq"),
        P("groups", "head", "seq"),
        P("groups", "head", "seq"),
        P("groups", "seq"),
        P("dim"),
    )
    out_specs = P("groups", "head", "dim", "seq")
    return jax.shard_map(local, mesh=mesh, in_specs=in_specs, out_specs=out_specs, check_vma=False)
```

```python
import jax
import jax.numpy as jnp
from jax import lax
from jax.experimental import pallas as pl
from jax.experimental.pallas import tpu as pltpu
from jax.sharding import PartitionSpec as P


F32 = jnp.float32
BF16 = jnp.bfloat16


def dot(left, right):
    return jnp.dot(left, right, preferred_element_type=F32)


def exact_dot(left, right):
    return jnp.dot(left, right, precision=lax.Precision.HIGH, preferred_element_type=F32)


def apply_map(left, right):
    return jnp.matmul(left, right, precision=lax.Precision.HIGH)


def passed(value, distance, first, last):
    return lax.ppermute(value, "seq", [(s, s + distance) for s in range(first, last)])


def split(full):
    high = full.astype(BF16)
    return high, (full - high.astype(F32)).astype(BF16)


def stack_rows(rows):
    blank = jnp.zeros_like(rows[0])
    return jnp.concatenate(rows + [blank] * (-len(rows) % 8), axis=0)


def state_kernel(
    lengths_in,
    key_in,
    value_in,
    beta_in,
    log_decay_in,
    query_in,
    gate_in,
    gain_in,
    end_out,
    mix_out,
    inv_out,
    fix_out,
    decay_out,
    keys_out,
    cum_out,
    live_out,
    key,
    query_out,
    gate_out,
    gain_out,
    value,
    lengths,
    high_ref,
    low_ref,
    beta,
    log_decay,
    sems,
):
    sources = [lengths_in, log_decay_in, beta_in, key_in, value_in, query_in, gate_in, gain_in]
    places = [lengths, log_decay, beta, key, value, query_out, gate_out, gain_out]
    copies = [pltpu.make_async_copy(s, p, sems.at[n]) for n, (s, p) in enumerate(zip(sources, places))]
    for copy in copies:
        copy.start()
    seqs, heads, tokens, width = key.shape
    half = tokens // 2
    pairs = [(b, h) for b in range(seqs) for h in range(heads)]
    count = len(pairs)
    lane = lax.broadcasted_iota(jnp.int32, (1, tokens), 1)
    row = lax.broadcasted_iota(jnp.int32, (tokens, tokens), 0)
    col = lax.broadcasted_iota(jnp.int32, (tokens, tokens), 1)
    ones = (row <= col).astype(BF16)
    low_row = lax.broadcasted_iota(jnp.int32, (half, half), 0)
    low_col = lax.broadcasted_iota(jnp.int32, (half, half), 1)
    apart = low_row ^ low_col
    low_eye = (low_row == low_col).astype(F32)
    wide_eye = jnp.concatenate([low_eye, jnp.zeros_like(low_eye)], axis=1)
    masks = [(apart < 4).astype(BF16)]
    size = 4
    while size < half:
        masks.append(((apart >= size) & (apart < 2 * size)).astype(BF16))
        size *= 2

    for copy in copies[:2]:
        copy.wait()
    live = [lane < lengths[0, b] for b, _ in pairs]
    live_out[...] = stack_rows([mask.astype(F32) for mask in live])
    decays = stack_rows([jnp.where(live[i], log_decay[b, pl.ds(h, 1), :], 0.0) for i, (b, h) in enumerate(pairs)])
    part0 = decays.astype(BF16)
    rest = decays - part0.astype(F32)
    part1 = rest.astype(BF16)
    part2 = (rest - part1.astype(F32)).astype(BF16)
    cum = dot(part0, ones) + (dot(part1, ones) + dot(part2, ones))
    cum_out[...] = cum

    for copy in copies[2:4]:
        copy.wait()
    keys_t, norms, shifts, weights, cums = [], [], [], [], []
    for i, (b, h) in enumerate(pairs):
        key_t = key[b, h].T
        wide = key_t.astype(F32)
        squares = jnp.sum(wide * wide, axis=0, keepdims=True) + 1e-06
        norm = lax.rsqrt(squares)
        c = cum[i : i + 1]
        rate = beta[b, pl.ds(h, 1), :]
        keys_t.append(key_t)
        norms.append(norm)
        cums.append(c)
        shifts.append(jnp.where(live[i], c + 0.5 * jnp.log(squares) - jnp.log(rate), 1e30))
        weights.append(jnp.where(live[i], rate * norm * jnp.exp(c[:, tokens - 1 :] - c), 0.0))
    columns = stack_rows(shifts + weights).T

    grams = [
        [
            dot(key[b, h, :half], keys_t[i]),
            dot(key[b, h, half:], keys_t[i][:, half:]),
        ]
        for i, (b, h) in enumerate(pairs)
    ]
    for i in range(count):
        shift = columns[:, i : i + 1]
        for r, c in ((0, 0), (0, half), (half, half)):
            gap = cums[i][:, c : c + half] - shift[r : r + half]
            if r == c:
                gap = jnp.where(low_row <= low_col, gap, -1e30)
            decay = jnp.exp(gap)
            decay_out[i, r : r + half, c : c + half] = decay
            gram = grams[i][1] if r else grams[i][0][:, c : c + half]
            link = gram * decay * norms[i][:, c : c + half]
            if r == c:
                link = jnp.where(low_row < low_col, link, 0.0)
            high, low = split(link)
            high_ref[i, r : r + half, c : c + half] = high
            low_ref[i, r : r + half, c : c + half] = low
        high_ref[i, half:, :half] = jnp.zeros((half, half), BF16)
        low_ref[i, half:, :half] = jnp.zeros((half, half), BF16)

    copies[4].wait()
    members = range(count)
    blocks = [(i, s) for i in members for s in (0, half)]
    steps = [high_ref[i, s : s + half, s : s + half] * masks[0] for i, s in blocks]
    twos = [dot(n, n) for n in steps]
    invs = [(low_eye - n.astype(F32) + t - dot(n, t.astype(BF16))).astype(BF16) for n, t in zip(steps, twos)]
    size = 4
    for mask in masks[1:]:
        links = [high_ref[i, s : s + half, s : s + half] * mask for i, s in blocks]
        if size < 16:
            mids = [dot(x, link).astype(BF16) for x, link in zip(invs, links)]
            invs = [x - dot(m, x).astype(BF16) for x, m in zip(invs, mids)]
        else:
            uppers = [jnp.concatenate([x[k : k + size] for k in range(0, half, 2 * size)], axis=0) for x in invs]
            mids = [dot(u, link).astype(BF16) for u, link in zip(uppers, links)]
            uppers = [u - dot(m, x).astype(BF16) for u, m, x in zip(uppers, mids, invs)]
            invs = [
                jnp.concatenate(
                    [
                        piece
                        for k in range(0, half, 2 * size)
                        for piece in (u[k // 2 : k // 2 + size], x[k + size : k + 2 * size])
                    ],
                    axis=0,
                )
                for u, x in zip(uppers, invs)
            ]
        size *= 2
    mids = [dot(invs[2 * i], high_ref[i, :half, half:]).astype(BF16) for i in members]
    corners = [-dot(mid, invs[2 * i + 1]).astype(BF16) for i, mid in enumerate(mids)]
    for i in members:
        inv_out[i, :half, :half] = invs[2 * i]
        inv_out[i, :half, half:] = corners[i]
        inv_out[i, half:, :half] = jnp.zeros_like(corners[i])
        inv_out[i, half:, half:] = invs[2 * i + 1]
    sides = [split(key[pairs[i]].astype(F32) * columns[:, count + i : count + i + 1]) for i in members]
    tops = [
        dot(
            jnp.concatenate([inv_out[i, :half], inv_out[i, :half]], axis=1),
            jnp.concatenate([high_ref[i], low_ref[i]], axis=0),
        )
        for i in members
    ]
    bottoms = [
        dot(
            jnp.concatenate([invs[2 * i + 1], invs[2 * i + 1]], axis=1),
            jnp.concatenate([high_ref[i, half:, half:], low_ref[i, half:, half:]], axis=0),
        )
        for i in members
    ]
    mixes = [dot(inv_out[i], jnp.concatenate(sides[i], axis=1)) for i in members]
    for i in members:
        fix_out[i, :half] = (wide_eye - inv_out[i, :half].astype(F32) - tops[i]).astype(BF16)
        fix_out[i, half:, :half] = jnp.zeros((half, half), BF16)
        fix_out[i, half:, half:] = (low_eye - invs[2 * i + 1].astype(F32) - bottoms[i]).astype(BF16)
    mixes = [mixed[:, :width] + mixed[:, width:] for mixed in mixes]
    parts = [split(mixed + dot(fix_out[i], mixed.astype(BF16))) for i, mixed in enumerate(mixes)]
    for i, (high, low) in enumerate(parts):
        end_out[pairs[i]] = from_values_narrow(value[pairs[i]], high, low)
        mix_out[i, 0] = high
        mix_out[i, 1] = low
    for i in members:
        key_high, key_low = split(keys_t[i].astype(F32) * (jnp.exp(cums[i]) * norms[i]))
        keys_out[i, 0] = key_high
        keys_out[i, 1] = key_low
    for copy in copies[5:]:
        copy.wait()


def from_values(value, high, low):
    return dot(jnp.concatenate([value, value], axis=1), jnp.concatenate([high, low], axis=0))


def from_values_narrow(value, high, low):
    both = dot(value, jnp.concatenate([high, low], axis=1))
    return both[:, : high.shape[1]] + both[:, high.shape[1] :]


def from_keys(key_high, key_low, high, low):
    return dot(
        jnp.concatenate([key_high, key_low, key_high], axis=1), jnp.concatenate([high, high, low], axis=0)
    )


def output_kernel(
    query, key, value, mix, inv, fix, decay, keys, cum, gate, gain, live, own_out, carry_out, map_out, factor_out
):
    seqs, heads, tokens, width = query.shape
    half = tokens // 2
    pairs = [(b, h) for b in range(seqs) for h in range(heads)]
    queries = [query[pair].T for pair in pairs]
    fixes = [dot(fix[i], inv[i]) for i in range(len(pairs))]
    tops = [dot(key[b, h, :half], query_t) for (b, h), query_t in zip(pairs, queries)]
    bottoms = [dot(key[b, h, half:], query_t[:, half:]) for (b, h), query_t in zip(pairs, queries)]
    parts = []
    for i, (top, bottom) in enumerate(zip(tops, bottoms)):
        bottom = bottom * decay[i, half:, half:]
        bottom = jnp.concatenate([jnp.zeros_like(bottom), bottom], axis=1)
        parts.append(split(jnp.concatenate([top * decay[i, :half], bottom], axis=0)))
    mixes = [
        dot(
            jnp.concatenate([inv[i], inv[i], fixes[i].astype(BF16)], axis=1),
            jnp.concatenate([high, low, high], axis=0),
        )
        for i, (high, low) in enumerate(parts)
    ]
    eye = (
        lax.broadcasted_iota(jnp.int32, (width, width), 0) == lax.broadcasted_iota(jnp.int32, (width, width), 1)
    ).astype(F32)
    for i, pair in enumerate(pairs):
        whole = jnp.exp(cum[i : i + 1, tokens - 1 :])
        both = from_values_narrow(keys[i, 0], mix[i, 0], mix[i, 1])
        map_out[pair] = whole * eye - (both + dot(keys[i, 1], mix[i, 0]))
    gains = jnp.broadcast_to(gain[...], (8, gain.shape[1])).T[:, :1]
    for i, pair in enumerate(pairs):
        opened = gate[pair].astype(F32)
        factor_out[pair] = gains * (opened / (1.0 + jnp.exp(-opened))) * live[i : i + 1]
    parts = [split(mixed) for mixed in mixes]
    for i, (high, low) in enumerate(parts):
        own_out[pairs[i]] = from_values(value[pairs[i]], high, low)
    for i, (high, low) in enumerate(parts):
        taken = from_keys(keys[i, 0], keys[i, 1], high, low)
        carry_out[pairs[i]] = queries[i].astype(F32) * jnp.exp(cum[i : i + 1]) - taken


def raw_kernel(own, carry, near, next_near, first, far, product, raw_out, square_out):
    seqs, heads = own.shape[:2]
    pairs = [(b, h) for b in range(seqs) for h in range(heads)]
    states = [(near[pair] + next_near[pair]) + exact_dot(first[pair] + far[pair], product[pair]) for pair in pairs]
    raws = [own[pair] + exact_dot(state, carry[pair]) for pair, state in zip(pairs, states)]
    for pair, raw in zip(pairs, raws):
        raw_out[pair] = raw
    square_out[...] = stack_rows([jnp.sum(raw * raw, axis=0, keepdims=True) for raw in raws])


def gate_kernel(raw, squares, factor, out):
    seqs, heads, val_width, _ = raw.shape
    total = jnp.sum(squares[...], axis=0)
    scale = lax.rsqrt(total / (val_width * squares.shape[0]) + 1e-06)
    for b in range(seqs):
        for h in range(heads):
            i = b * heads + h
            out[b, h] = (raw[b, h] * scale[i : i + 1] * factor[b, h]).astype(BF16)


VMEM = pl.BlockSpec(memory_space=pltpu.VMEM)


def call(body, outs, *operands, space=VMEM, scratch=()):
    return pl.pallas_call(
        body,
        out_shape=outs,
        in_specs=[space] * len(operands),
        out_specs=jax.tree.map(lambda _: VMEM, outs),
        scratch_shapes=scratch,
        compiler_params=pltpu.CompilerParams(vmem_limit_bytes=16 * 1024 * 1024),
    )(*operands)


def local(query, key, value, out_gate, beta, log_decay, lengths, norm_gain):
    seqs, heads, tokens, width = query.shape
    val_width = value.shape[2]
    count = seqs * heads
    shape = jax.ShapeDtypeStruct
    rows = shape((count + -count % 8, tokens), F32)
    lengths = lengths.T
    norm_gain = norm_gain[None, :]
    block_end, mix, inverse, fix, decay, keys, cum, live, key, query, out_gate, norm_gain, value = call(
        state_kernel,
        (
            shape((seqs, heads, val_width, width), F32),
            shape((count, 2, tokens, width), BF16),
            shape((count, tokens, tokens), BF16),
            shape((count, tokens, tokens), BF16),
            shape((count, tokens, tokens), F32),
            shape((count, 2, width, tokens), BF16),
            rows,
            rows,
            shape(key.shape, BF16),
            shape(query.shape, BF16),
            shape(out_gate.shape, BF16),
            shape(norm_gain.shape, F32),
            shape(value.shape, BF16),
        ),
        *[
            pltpu.with_memory_space_constraint(array, pltpu.HBM)
            for array in (lengths, key, value, beta, log_decay, query, out_gate, norm_gain)
        ],
        space=pl.BlockSpec(memory_space=pltpu.HBM),
        scratch=[
            pltpu.SMEM(lengths.shape, jnp.int32),
            pltpu.VMEM((count, tokens, tokens), BF16),
            pltpu.VMEM((count, tokens, tokens), BF16),
            pltpu.VMEM(beta.shape, F32),
            pltpu.VMEM(log_decay.shape, F32),
            pltpu.SemaphoreType.DMA((8,)),
        ],
    )
    steps = lax.axis_size("seq")
    near = passed(block_end, 1, 0, steps - 1)
    first = passed(block_end, 3, 0, 1)
    own, carry, block_map, factor = call(
        output_kernel,
        (
            shape((seqs, heads, val_width, tokens), F32),
            shape((seqs, heads, width, tokens), F32),
            shape((seqs, heads, width, width), F32),
            shape((seqs, heads, val_width, tokens), F32),
        ),
        query,
        key,
        value,
        mix,
        inverse,
        fix,
        decay,
        keys,
        cum,
        out_gate,
        norm_gain,
        live,
    )
    moved = apply_map(near, block_map)
    far = passed(block_end + moved, 3, 1, steps - 3)
    next_near = passed(moved, 1, 1, steps - 1)
    earlier = passed(block_map, 1, 1, steps - 2)
    product = passed(apply_map(earlier, block_map), 1, 2, steps - 1)
    raw, squares = call(
        raw_kernel,
        (shape((seqs, heads, val_width, tokens), F32), rows),
        own,
        carry,
        near,
        next_near,
        first,
        far,
        product,
    )
    squares = lax.all_gather(squares, "dim")
    return call(
        gate_kernel,
        shape((seqs, heads, val_width, tokens), BF16),
        raw,
        squares,
        factor,
    )


def solution(mesh):
    in_specs = (
        P("groups", "head", "seq", None),
        P("groups", "head", "seq", None),
        P("groups", "head", "dim", "seq"),
        P("groups", "head", "dim", "seq"),
        P("groups", "head", "seq"),
        P("groups", "head", "seq"),
        P("groups", "seq"),
        P("dim"),
    )
    out_specs = P("groups", "head", "dim", "seq")
    return jax.shard_map(local, mesh=mesh, in_specs=in_specs, out_specs=out_specs, check_vma=False)
```

```python
import jax
import jax.numpy as jnp
from jax import lax
from jax.experimental import pallas as pl
from jax.experimental.pallas import tpu as pltpu
from jax.sharding import PartitionSpec as P


F32 = jnp.float32
BF16 = jnp.bfloat16


def dot(left, right):
    return jnp.dot(left, right, preferred_element_type=F32)


def exact_dot(left, right):
    return jnp.dot(left, right, precision=lax.Precision.HIGH, preferred_element_type=F32)


def apply_map(left, right):
    return jnp.matmul(left, right, precision=lax.Precision.HIGH)


def passed(value, distance, first, last):
    return lax.ppermute(value, "seq", [(s, s + distance) for s in range(first, last)])


def split(full):
    high = full.astype(BF16)
    return high, (full - high.astype(F32)).astype(BF16)


def stack_rows(rows):
    blank = jnp.zeros_like(rows[0])
    return jnp.concatenate(rows + [blank] * (-len(rows) % 8), axis=0)


def state_kernel(
    lengths_in,
    key_in,
    value_in,
    beta_in,
    log_decay_in,
    query_in,
    gate_in,
    gain_in,
    end_out,
    mix_out,
    inv_out,
    fix_out,
    decay_out,
    keys_out,
    cum_out,
    live_out,
    key,
    query_out,
    gate_out,
    gain_out,
    value,
    lengths,
    high_ref,
    low_ref,
    beta,
    log_decay,
    sems,
):
    sources = [lengths_in, log_decay_in, beta_in, key_in, value_in, query_in, gate_in, gain_in]
    places = [lengths, log_decay, beta, key, value, query_out, gate_out, gain_out]
    copies = [pltpu.make_async_copy(s, p, sems.at[n]) for n, (s, p) in enumerate(zip(sources, places))]
    for copy in copies:
        copy.start()
    seqs, heads, tokens, width = key.shape
    half = tokens // 2
    pairs = [(b, h) for b in range(seqs) for h in range(heads)]
    count = len(pairs)
    lane = lax.broadcasted_iota(jnp.int32, (1, tokens), 1)
    row = lax.broadcasted_iota(jnp.int32, (tokens, tokens), 0)
    col = lax.broadcasted_iota(jnp.int32, (tokens, tokens), 1)
    ones = (row <= col).astype(BF16)
    low_row = lax.broadcasted_iota(jnp.int32, (half, half), 0)
    low_col = lax.broadcasted_iota(jnp.int32, (half, half), 1)
    apart = low_row ^ low_col
    low_eye = (low_row == low_col).astype(F32)
    wide_eye = jnp.concatenate([low_eye, jnp.zeros_like(low_eye)], axis=1)
    masks = [(apart < 4).astype(BF16)]
    size = 4
    while size < half:
        masks.append(((apart >= size) & (apart < 2 * size)).astype(BF16))
        size *= 2

    for ref in (high_ref, low_ref, inv_out, fix_out):
        for i in range(count):
            ref[i, half:, :half] = jnp.zeros((half, half), BF16)
    for copy in copies[:2]:
        copy.wait()
    live = [lane < lengths[0, b] for b, _ in pairs]
    live_out[...] = stack_rows([mask.astype(F32) for mask in live])
    decays = stack_rows([jnp.where(live[i], log_decay[b, pl.ds(h, 1), :], 0.0) for i, (b, h) in enumerate(pairs)])
    part0 = decays.astype(BF16)
    rest = decays - part0.astype(F32)
    part1 = rest.astype(BF16)
    part2 = (rest - part1.astype(F32)).astype(BF16)
    cum = dot(part0, ones) + (dot(part1, ones) + dot(part2, ones))
    cum_out[...] = cum

    for copy in copies[2:4]:
        copy.wait()
    keys_t, norms, shifts, weights, cums = [], [], [], [], []
    for i, (b, h) in enumerate(pairs):
        key_t = key[b, h].T
        wide = key_t.astype(F32)
        squares = jnp.sum(wide * wide, axis=0, keepdims=True) + 1e-06
        norm = lax.rsqrt(squares)
        c = cum[i : i + 1]
        rate = beta[b, pl.ds(h, 1), :]
        keys_t.append(key_t)
        norms.append(norm)
        cums.append(c)
        shifts.append(jnp.where(live[i], c + 0.5 * jnp.log(squares) - jnp.log(rate), 1e30))
        weights.append(jnp.where(live[i], rate * norm * jnp.exp(c[:, tokens - 1 :] - c), 0.0))
    columns = stack_rows(shifts + weights).T

    grams = [
        [
            dot(key[b, h, :half], keys_t[i]),
            dot(key[b, h, half:], keys_t[i][:, half:]),
        ]
        for i, (b, h) in enumerate(pairs)
    ]
    for i in range(count):
        shift = columns[:, i : i + 1]
        for r, c in ((0, 0), (0, half), (half, half)):
            gap = cums[i][:, c : c + half] - shift[r : r + half]
            if r == c:
                gap = jnp.where(low_row <= low_col, gap, -1e30)
            decay = jnp.exp(gap)
            decay_out[i, r : r + half, c : c + half] = decay
            gram = grams[i][1] if r else grams[i][0][:, c : c + half]
            link = gram * decay * norms[i][:, c : c + half]
            if r == c:
                link = jnp.where(low_row < low_col, link, 0.0)
            high, low = split(link)
            high_ref[i, r : r + half, c : c + half] = high
            low_ref[i, r : r + half, c : c + half] = low
    copies[4].wait()
    members = range(count)
    blocks = [(i, s) for i in members for s in (0, half)]
    steps = [high_ref[i, s : s + half, s : s + half] * masks[0] for i, s in blocks]
    twos = [dot(n, n) for n in steps]
    invs = [(low_eye - n.astype(F32) + t - dot(n, t.astype(BF16))).astype(BF16) for n, t in zip(steps, twos)]
    size = 4
    for mask in masks[1:]:
        links = [high_ref[i, s : s + half, s : s + half] * mask for i, s in blocks]
        if size < 16:
            mids = [dot(x, link).astype(BF16) for x, link in zip(invs, links)]
            invs = [x - dot(m, x).astype(BF16) for x, m in zip(invs, mids)]
        else:
            uppers = [jnp.concatenate([x[k : k + size] for k in range(0, half, 2 * size)], axis=0) for x in invs]
            mids = [dot(u, link).astype(BF16) for u, link in zip(uppers, links)]
            uppers = [u - dot(m, x).astype(BF16) for u, m, x in zip(uppers, mids, invs)]
            invs = [
                jnp.concatenate(
                    [
                        piece
                        for k in range(0, half, 2 * size)
                        for piece in (u[k // 2 : k // 2 + size], x[k + size : k + 2 * size])
                    ],
                    axis=0,
                )
                for u, x in zip(uppers, invs)
            ]
        size *= 2
    mids = [dot(invs[2 * i], high_ref[i, :half, half:]).astype(BF16) for i in members]
    corners = [-dot(mid, invs[2 * i + 1]).astype(BF16) for i, mid in enumerate(mids)]
    for i in members:
        inv_out[i, :half, :half] = invs[2 * i]
        inv_out[i, :half, half:] = corners[i]
        inv_out[i, half:, half:] = invs[2 * i + 1]
    sides = [split(key[pairs[i]].astype(F32) * columns[:, count + i : count + i + 1]) for i in members]
    tops = [
        dot(
            jnp.concatenate([inv_out[i, :half], inv_out[i, :half]], axis=1),
            jnp.concatenate([high_ref[i], low_ref[i]], axis=0),
        )
        for i in members
    ]
    bottoms = [
        dot(
            jnp.concatenate([invs[2 * i + 1], invs[2 * i + 1]], axis=1),
            jnp.concatenate([high_ref[i, half:, half:], low_ref[i, half:, half:]], axis=0),
        )
        for i in members
    ]
    mixes = [dot(inv_out[i], jnp.concatenate(sides[i], axis=1)) for i in members]
    for i in members:
        fix_out[i, :half] = (wide_eye - inv_out[i, :half].astype(F32) - tops[i]).astype(BF16)
        fix_out[i, half:, half:] = (low_eye - invs[2 * i + 1].astype(F32) - bottoms[i]).astype(BF16)
    mixes = [mixed[:, :width] + mixed[:, width:] for mixed in mixes]
    parts = [split(mixed + dot(fix_out[i], mixed.astype(BF16))) for i, mixed in enumerate(mixes)]
    for i, (high, low) in enumerate(parts):
        end_out[pairs[i]] = from_values_narrow(value[pairs[i]], high, low)
        mix_out[i, 0] = high
        mix_out[i, 1] = low
    for i in members:
        key_high, key_low = split(keys_t[i].astype(F32) * (jnp.exp(cums[i]) * norms[i]))
        keys_out[i, 0] = key_high
        keys_out[i, 1] = key_low
    for copy in copies[5:]:
        copy.wait()


def from_values(value, high, low):
    return dot(jnp.concatenate([value, value], axis=1), jnp.concatenate([high, low], axis=0))


def from_values_narrow(value, high, low):
    both = dot(value, jnp.concatenate([high, low], axis=1))
    return both[:, : high.shape[1]] + both[:, high.shape[1] :]


def from_keys(key_high, key_low, high, low):
    return dot(
        jnp.concatenate([key_high, key_low, key_high], axis=1), jnp.concatenate([high, high, low], axis=0)
    )


def output_kernel(
    query, key, value, mix, inv, fix, decay, keys, cum, gate, gain, live, own_out, carry_out, map_out, factor_out
):
    seqs, heads, tokens, width = query.shape
    half = tokens // 2
    pairs = [(b, h) for b in range(seqs) for h in range(heads)]
    queries = [query[pair].T for pair in pairs]
    fixes = [dot(fix[i], inv[i]) for i in range(len(pairs))]
    tops = [dot(key[b, h, :half], query_t) for (b, h), query_t in zip(pairs, queries)]
    bottoms = [dot(key[b, h, half:], query_t[:, half:]) for (b, h), query_t in zip(pairs, queries)]
    parts = []
    for i, (top, bottom) in enumerate(zip(tops, bottoms)):
        bottom = bottom * decay[i, half:, half:]
        bottom = jnp.concatenate([jnp.zeros_like(bottom), bottom], axis=1)
        parts.append(split(jnp.concatenate([top * decay[i, :half], bottom], axis=0)))
    fixes = [fixed.astype(BF16) for fixed in fixes]
    wides = [
        dot(
            jnp.concatenate([inv[i, :half], inv[i, :half], fixes[i][:half]], axis=1),
            jnp.concatenate([high, low, high], axis=0),
        )
        for i, (high, low) in enumerate(parts)
    ]
    corners = [
        dot(
            jnp.concatenate([inv[i, half:, half:], inv[i, half:, half:], fixes[i][half:, half:]], axis=1),
            jnp.concatenate([high[half:, half:], low[half:, half:], high[half:, half:]], axis=0),
        )
        for i, (high, low) in enumerate(parts)
    ]
    mixes = [
        jnp.concatenate([wide, jnp.concatenate([jnp.zeros_like(corner), corner], axis=1)], axis=0)
        for wide, corner in zip(wides, corners)
    ]
    eye = (
        lax.broadcasted_iota(jnp.int32, (width, width), 0) == lax.broadcasted_iota(jnp.int32, (width, width), 1)
    ).astype(F32)
    for i, pair in enumerate(pairs):
        whole = jnp.exp(cum[i : i + 1, tokens - 1 :])
        both = from_values_narrow(keys[i, 0], mix[i, 0], mix[i, 1])
        map_out[pair] = whole * eye - (both + dot(keys[i, 1], mix[i, 0]))
    gains = jnp.broadcast_to(gain[...], (8, gain.shape[1])).T[:, :1]
    for i, pair in enumerate(pairs):
        opened = gate[pair].astype(F32)
        factor_out[pair] = gains * (opened / (1.0 + jnp.exp(-opened))) * live[i : i + 1]
    parts = [split(mixed) for mixed in mixes]
    for i, (high, low) in enumerate(parts):
        own_out[pairs[i]] = from_values(value[pairs[i]], high, low)
    for i, (high, low) in enumerate(parts):
        taken = from_keys(keys[i, 0], keys[i, 1], high, low)
        carry_out[pairs[i]] = queries[i].astype(F32) * jnp.exp(cum[i : i + 1]) - taken


def raw_kernel(own, carry, near, next_near, first, far, product, raw_out, square_out):
    seqs, heads = own.shape[:2]
    pairs = [(b, h) for b in range(seqs) for h in range(heads)]
    states = [(near[pair] + next_near[pair]) + exact_dot(first[pair] + far[pair], product[pair]) for pair in pairs]
    raws = [own[pair] + exact_dot(state, carry[pair]) for pair, state in zip(pairs, states)]
    for pair, raw in zip(pairs, raws):
        raw_out[pair] = raw
    square_out[...] = stack_rows([jnp.sum(raw * raw, axis=0, keepdims=True) for raw in raws])


def gate_kernel(raw, squares, factor, out):
    seqs, heads, val_width, _ = raw.shape
    total = jnp.sum(squares[...], axis=0)
    scale = lax.rsqrt(total / (val_width * squares.shape[0]) + 1e-06)
    for b in range(seqs):
        for h in range(heads):
            i = b * heads + h
            out[b, h] = (raw[b, h] * scale[i : i + 1] * factor[b, h]).astype(BF16)


VMEM = pl.BlockSpec(memory_space=pltpu.VMEM)


def call(body, outs, *operands, space=VMEM, scratch=()):
    return pl.pallas_call(
        body,
        out_shape=outs,
        in_specs=[space] * len(operands),
        out_specs=jax.tree.map(lambda _: VMEM, outs),
        scratch_shapes=scratch,
        compiler_params=pltpu.CompilerParams(vmem_limit_bytes=16 * 1024 * 1024),
    )(*operands)


def local(query, key, value, out_gate, beta, log_decay, lengths, norm_gain):
    seqs, heads, tokens, width = query.shape
    val_width = value.shape[2]
    count = seqs * heads
    shape = jax.ShapeDtypeStruct
    rows = shape((count + -count % 8, tokens), F32)
    lengths = lengths.T
    norm_gain = norm_gain[None, :]
    block_end, mix, inverse, fix, decay, keys, cum, live, key, query, out_gate, norm_gain, value = call(
        state_kernel,
        (
            shape((seqs, heads, val_width, width), F32),
            shape((count, 2, tokens, width), BF16),
            shape((count, tokens, tokens), BF16),
            shape((count, tokens, tokens), BF16),
            shape((count, tokens, tokens), F32),
            shape((count, 2, width, tokens), BF16),
            rows,
            rows,
            shape(key.shape, BF16),
            shape(query.shape, BF16),
            shape(out_gate.shape, BF16),
            shape(norm_gain.shape, F32),
            shape(value.shape, BF16),
        ),
        *[
            pltpu.with_memory_space_constraint(array, pltpu.HBM)
            for array in (lengths, key, value, beta, log_decay, query, out_gate, norm_gain)
        ],
        space=pl.BlockSpec(memory_space=pltpu.HBM),
        scratch=[
            pltpu.SMEM(lengths.shape, jnp.int32),
            pltpu.VMEM((count, tokens, tokens), BF16),
            pltpu.VMEM((count, tokens, tokens), BF16),
            pltpu.VMEM(beta.shape, F32),
            pltpu.VMEM(log_decay.shape, F32),
            pltpu.SemaphoreType.DMA((8,)),
        ],
    )
    steps = lax.axis_size("seq")
    near = passed(block_end, 1, 0, steps - 1)
    first = passed(block_end, 3, 0, 1)
    own, carry, block_map, factor = call(
        output_kernel,
        (
            shape((seqs, heads, val_width, tokens), F32),
            shape((seqs, heads, width, tokens), F32),
            shape((seqs, heads, width, width), F32),
            shape((seqs, heads, val_width, tokens), F32),
        ),
        query,
        key,
        value,
        mix,
        inverse,
        fix,
        decay,
        keys,
        cum,
        out_gate,
        norm_gain,
        live,
    )
    moved = apply_map(near, block_map)
    far = passed(block_end + moved, 3, 1, steps - 3)
    next_near = passed(moved, 1, 1, steps - 1)
    earlier = passed(block_map, 1, 1, steps - 2)
    product = passed(apply_map(earlier, block_map), 1, 2, steps - 1)
    raw, squares = call(
        raw_kernel,
        (shape((seqs, heads, val_width, tokens), F32), rows),
        own,
        carry,
        near,
        next_near,
        first,
        far,
        product,
    )
    squares = lax.all_gather(squares, "dim")
    return call(
        gate_kernel,
        shape((seqs, heads, val_width, tokens), BF16),
        raw,
        squares,
        factor,
    )


def solution(mesh):
    in_specs = (
        P("groups", "head", "seq", None),
        P("groups", "head", "seq", None),
        P("groups", "head", "dim", "seq"),
        P("groups", "head", "dim", "seq"),
        P("groups", "head", "seq"),
        P("groups", "head", "seq"),
        P("groups", "seq"),
        P("dim"),
    )
    out_specs = P("groups", "head", "dim", "seq")
    return jax.shard_map(local, mesh=mesh, in_specs=in_specs, out_specs=out_specs, check_vma=False)
```
